128 devices in a mesh: expert: 4 (over y), shard: 32 (over z, x, core).
Axes of the slice: x: 4, y: 4, z: 4, core: 2. Of those that a mesh axis runs over, the one named last changes fastest.
Arguments:
- master_gate: float32 [64, 2048, 1408], P('expert', 'shard'), may hold values from -0.25 to 0.25
- master_up: float32 [64, 2048, 1408], P('expert', 'shard'), may hold values from -0.25 to 0.25
- master_down: float32 [64, 1408, 2048], P('expert', None, 'shard'), may hold values from -0.3125 to 0.3125
- router_weight: float32 [2048, 64], P('shard', 'expert'), may hold values from -0.125 to 0.125
- router_gain: float32 [2048], P('shard'), may hold values from 0.25 to 1.75
Outputs:
- final_gate: bfloat16 [64, 2048, 1408], P('expert', None, 'shard')
- final_up: bfloat16 [64, 2048, 1408], P('expert', None, 'shard')
- final_down: bfloat16 [64, 1408, 2048], P('expert', 'shard')
- scale_gate: float32 [64, 1408], P('expert', 'shard')
- scale_up: float32 [64, 1408], P('expert', 'shard')
- scale_down: float32 [64, 1408], P('expert', 'shard')
- serve_router: bfloat16 [2048, 64], replicated
The draws below stay inside these ranges and needn't reach their ends.
All inputs are finite; a program needn't handle non-finite values. Where the reference program divides by a largest or mean magnitude, that divisor is 1e-20 or more.
Results may differ from the reference program's by a relative error of at most 0.001.
Values may be sent and summed in bfloat16 or wider, within the bound.
No kernel may reach another device: no remote copies, remote signals or barrier semaphores. Data moves between devices by JAX's collectives and lax.ppermute only.
A program may use at most 192 MiB of HBM per device.

```python
import jax
import jax.numpy as jnp

EXPERTS = 64
D_MODEL = 2048
D_EXPERT = 1408


def with_spikes(drawn, stream_key, source, target, shards_of, factor):
    owner, partner = [(jnp.arange(drawn.shape[position]) // (drawn.shape[position] // shards_of)).reshape([-1 if axis == position else 1 for axis in range(drawn.ndim)]) for position in (source, target)]
    chosen = jax.random.permutation(stream_key, shards_of)[partner]
    strong = (owner == chosen) | (owner == (partner + shards_of // 2) % shards_of)
    return jnp.where(strong, factor * drawn, drawn)


def shard_levels(rng, dims, cuts, low, largest):
    def one(axis_at, blocks):
        heights = jax.random.uniform(jax.random.fold_in(jax.random.fold_in(rng, 6), axis_at), (blocks,), jnp.float32, low / len(cuts), largest / len(cuts))
        return jnp.repeat(jnp.exp(heights), dims[axis_at] // blocks).reshape((-1,) + (1,) * (len(dims) - axis_at - 1))

    gain = one(*cuts[0])
    for cut in cuts[1:]:
        gain = gain * one(*cut)
    return gain


def bell_draw(key, shape, scale, bound, cuts=(), kind=jnp.bfloat16):
    values = jax.random.normal(key, shape, jnp.float32) * scale
    if len(cuts) > 0:
        values = shard_levels(key, shape, cuts, -0.22, 0.18) * values
    return jnp.clip(values, min=-bound, max=bound).astype(kind)


def bell_draw_with(stream_key, shape, scale, most, split, heavy, held_as=jnp.bfloat16):
    array = scale * jax.random.normal(stream_key, shape, jnp.float32)
    if split:
        array = array * shard_levels(stream_key, shape, split, -0.22, 0.18)
    return jnp.clip(with_spikes(array, jax.random.fold_in(stream_key, 3), *heavy), -most, most).astype(held_as)


def setup_inputs(seed: int = 0) -> dict:
    key_list = jax.random.split(jax.random.key(seed), 6)
    master_gate = bell_draw_with(key_list[0], (EXPERTS, D_MODEL, D_EXPERT), D_MODEL ** -0.5, 0.25, ((0, 4), (1, 32)), (1, 2, 32, 2.75), jnp.float32)
    master_up = bell_draw_with(key_list[1], (EXPERTS, D_MODEL, D_EXPERT), D_MODEL ** -0.5, 0.25, ((0, 4), (1, 32)), (1, 2, 32, 2.75), jnp.float32)
    master_down = bell_draw_with(key_list[2], (EXPERTS, D_EXPERT, D_MODEL), D_EXPERT ** -0.5, 0.3125, ((0, 4), (2, 32)), (2, 1, 32, 2.75), jnp.float32)
    router_weight = bell_draw(key_list[3], (D_MODEL, EXPERTS), D_MODEL ** -0.5, 0.125, ((0, 32), (1, 4)), jnp.float32)
    router_gain = jnp.clip(1.0 + 0.15 * jax.random.normal(key_list[4], (D_MODEL,), jnp.float32), 0.25, 1.75)
    return dict(master_gate=master_gate, master_up=master_up, master_down=master_down, router_weight=router_weight, router_gain=router_gain)


def reference(master_gate, master_up, master_down, router_weight, router_gain):
    scale_gate = jnp.max(jnp.abs(master_gate), axis=1)
    final_gate = (master_gate / jnp.expand_dims(scale_gate, 1)).astype(jnp.bfloat16)
    scale_up = jnp.max(jnp.abs(master_up), axis=1)
    final_up = (master_up / jnp.expand_dims(scale_up, 1)).astype(jnp.bfloat16)
    scale_down = jnp.max(jnp.abs(master_down), axis=2)
    final_down = (master_down / jnp.expand_dims(scale_down, 2)).astype(jnp.bfloat16)
    serve_router = (router_weight * router_gain[:, None]).astype(jnp.bfloat16)
    return final_gate, final_up, final_down, scale_gate, scale_up, scale_down, serve_router
```

```python
import functools

import jax
import jax.numpy as jnp
from jax import lax
from jax.experimental import pallas as pl
from jax.experimental.pallas import tpu as pltpu
from jax.sharding import PartitionSpec as P


SPAN = 125.0
TINY = 1e-30
E = 16
F = 1408
M = 64
FD = 44
DEV = 32
LANES = 128
ROWS = FD * 8
PITCH = 9
VMEM = 56 * 2**20


def iota(shape, dim):
    return lax.broadcasted_iota(jnp.int32, shape, dim)


def encode_kernel(*refs, count, router):
    xs, refs = refs[:count], refs[count:]
    if router:
        weight, gain, refs = refs[0], refs[1], refs[2:]
    wire, xbuf, scr0, scr1, packed, tops, meta, isem, osem, msem, *refs = refs
    spans = [(at, min(256, F - at)) for at in range(0, F, 256)]

    def brought(a, i):
        part = pl.ds(*spans[i])
        return pltpu.make_async_copy(xs[a].at[:, :, part], xbuf.at[a, :, :, part], isem.at[a, i])

    for a in range(count):
        for i in range(len(spans)):
            brought(a, i).start()
    if router:
        wbuf, gbuf, wsem, gsem = refs
        wcopy = pltpu.make_async_copy(weight, wbuf, wsem)
        gcopy = pltpu.make_async_copy(gain, gbuf, gsem)
        wcopy.start()
        gcopy.start()
    eye = (iota((256, 256), 0) == iota((256, 256), 1)).astype(jnp.bfloat16)

    def code(a, at, width, scr):
        for p in range(0, 8, 2):
            rows = []
            for e in (p, p + 8, p + 1, p + 9):
                v = xbuf[a, e, :, at : at + width]
                top = jnp.maximum(jnp.max(jnp.abs(v), axis=0, keepdims=True), TINY)
                tops[a, e : e + 1, at : at + width] = top
                rows.append(jnp.exp2(v * (SPAN / top)).astype(jnp.bfloat16))
            turned = lax.dot_general(
                eye[:width, :width],
                jnp.concatenate(rows, axis=0),
                (((1,), (1,)), ((), ())),
                preferred_element_type=jnp.float32,
            )
            for n in range(width // LANES):
                for q in range(2):
                    scr[pl.ds(n * LANES * PITCH + p + q, LANES, stride=PITCH), :] = turned[
                        LANES * n : LANES * n + LANES, LANES * q : LANES * q + LANES
                    ]

    def pack(a, at, width, scr):
        for f in range(0, width, 2):
            pair = [scr[PITCH * g : PITCH * g + 8, :] for g in (f, f + 1)]
            packed[a, 8 * (at + f) : 8 * (at + f) + 16, :] = jnp.concatenate(pair, axis=0).astype(jnp.bfloat16)
        for d in range(at // FD, (at + width) // FD):
            pltpu.make_async_copy(
                packed.at[a, pl.ds(d * ROWS, ROWS), :], wire.at[d, pl.ds(a * ROWS, ROWS), :], osem
            ).start()

    def whole(a):
        last = None
        for i, (at, width) in enumerate(spans):
            brought(a, i).wait()
            scr = (scr0, scr1)[i % 2]
            code(a, at, width, scr)
            if last is not None:
                pack(*last)
            last = (a, at, width, scr)
        pack(*last)

    lane = iota((E, LANES), 1)

    for a in range(count):
        whole(a)
        for d in range(DEV):
            j, off = divmod(FD * d, LANES)
            near = tops[a, :, LANES * j : LANES * j + LANES]
            near = pltpu.roll(near, LANES - off, 1) if off else near
            if off + FD > LANES:
                far = pltpu.roll(tops[a, :, LANES * j + LANES : LANES * j + 2 * LANES], LANES - off, 1)
                near = jnp.where(lane < LANES - off, near, far)
            high = near.astype(jnp.bfloat16).astype(jnp.float32)
            rest = pltpu.roll(near - high, FD, 1)
            meta[d, E * a : E * a + E, :] = jnp.where(lane < FD, high, rest).astype(jnp.bfloat16)
    if router:
        wcopy.wait()
        gcopy.wait()
        r = wbuf[...] * gbuf[...]
        tile = jnp.concatenate([r[0:8], r[8:16]], axis=1).astype(jnp.bfloat16)
        for d in range(DEV):
            meta[d, E * count : E * count + 8, :] = tile
    rows = meta.shape[1]
    meta_copy = pltpu.make_async_copy(meta, wire.at[:, pl.ds(count * ROWS, rows), :], msem)
    meta_copy.start()
    pltpu.make_async_copy(packed, packed, osem).wait()
    meta_copy.wait()


def encode(xs, router=()):
    count = len(xs)
    rows = E * count + (8 if router else 0)
    hbm = pl.BlockSpec(memory_space=pl.ANY)
    small = [pltpu.VMEM(r.shape, r.dtype) for r in router] + [pltpu.SemaphoreType.DMA] * len(router)
    return pl.pallas_call(
        functools.partial(encode_kernel, count=count, router=bool(router)),
        in_specs=[hbm] * (count + len(router)),
        out_specs=hbm,
        out_shape=jax.ShapeDtypeStruct((DEV, count * ROWS + rows, LANES), jnp.bfloat16),
        scratch_shapes=[
            pltpu.VMEM((count, E, M, F), jnp.float32),
            pltpu.VMEM((256 * PITCH, LANES), jnp.float32),
            pltpu.VMEM((256 * PITCH, LANES), jnp.float32),
            pltpu.VMEM((count, F * 8, LANES), jnp.bfloat16),
            pltpu.VMEM((count, E, F), jnp.float32),
            pltpu.VMEM((DEV, rows, LANES), jnp.bfloat16),
            pltpu.SemaphoreType.DMA((count, pl.cdiv(F, 256))),
            pltpu.SemaphoreType.DMA,
            pltpu.SemaphoreType.DMA,
            *small,
        ],
        compiler_params=pltpu.CompilerParams(vmem_limit_bytes=VMEM),
        name="encode",
    )(*xs, *router)


STEP = 4
STEPS = FD // STEP


def decode_kernel(*refs, count, router, near):
    wire, finals, scales, refs = refs[0], refs[1 : 1 + count], refs[1 + count : 1 + 2 * count], refs[1 + 2 * count :]
    if router:
        routed, refs = refs[0], refs[1:]
    obuf, share, select, order, osem, *refs = refs
    tail = count * ROWS
    if near:
        mbuf, base = wire, tail
    else:
        rbuf, mbuf, isem, msem = refs
        base = 0
        meta_copy = pltpu.make_async_copy(wire.at[:, pl.ds(tail, mbuf.shape[1]), :], mbuf, msem)
        meta_copy.start()
        for c in range(STEPS):
            for a in range(count):
                part = pl.ds(a * ROWS + c * STEP * 8, STEP * 8)
                pltpu.make_async_copy(wire.at[:, part, :], rbuf.at[c, a], isem.at[c]).start()
    k, n = iota((256, 256), 0), iota((256, 256), 1)
    source = (n & 63) + jnp.where((n & 64) == 0, 0, LANES) + jnp.where(n < LANES, 0, M)
    order[...] = jnp.where(k == source, 1.0, 0.0).astype(jnp.bfloat16)
    select[...] = (k & 127) - jnp.where((n & 64) == 0, 0, M) - jnp.where(n < LANES, 0, 1)
    if not near:
        meta_copy.wait()

    def top_of(s, a):
        v = mbuf[s, base + E * a : base + E * a + E, :].astype(jnp.float32)
        return v + pltpu.roll(v, LANES - FD, 1)

    low = iota((E, LANES), 1) < M
    for a in range(count):
        top = top_of(0, a)
        for s in range(1, DEV):
            top = jnp.maximum(top, top_of(s, a))
        scales[a][...] = top[:, :FD]
        inv = 1.0 / (SPAN * jnp.maximum(top, TINY))
        for b in range(DEV // 2):
            one = top_of(2 * b, a) * inv
            two = top_of(2 * b + 1, a) * inv
            part = jnp.where(low, one, pltpu.roll(two, M, 1))
            high = part.astype(jnp.bfloat16)
            at = 256 * a + E * b
            share[at : at + E, 0:LANES] = high
            share[at : at + E, LANES : 2 * LANES] = (part - high.astype(jnp.float32)).astype(jnp.bfloat16)
    if router:
        at = base + E * count
        for b in range(DEV // 2):
            one = mbuf[2 * b, at : at + 8, :].astype(jnp.float32)
            two = mbuf[2 * b + 1, at : at + 8, :].astype(jnp.float32)
            first = jnp.where(low[0:8], one, pltpu.roll(two, M, 1))
            second = jnp.where(low[0:8], pltpu.roll(one, M, 1), two)
            routed[:, LANES * b : LANES * b + LANES] = jnp.concatenate([first, second], axis=0).astype(jnp.bfloat16)

    def codes_of(c, a, i, s):
        if near:
            return wire[s, pl.ds(pl.multiple_of(a * ROWS + 8 * (c * STEP + i), 16), 16), :]
        return rbuf[c, a, s, 8 * i : 8 * i + 16, :]

    def step(c, carry):
        if not near:
            pltpu.make_async_copy(rbuf.at[c], rbuf.at[c], isem.at[c]).wait()
        rows = [
            jnp.concatenate([codes_of(c, a, i, 2 * b + q) for q in range(2)], axis=1)
            for i in range(0, STEP, 2)
            for a in range(count)
            for b in range(DEV // 2)
        ]
        logs = jnp.log2(jnp.dot(jnp.concatenate(rows, axis=0), order[...], preferred_element_type=jnp.float32))
        for i in range(0, STEP, 2):
            pick = jnp.where(select[...] == c * STEP + i, 1.0, 0.0).astype(jnp.bfloat16)
            factor = jnp.dot(share[...], pick, preferred_element_type=jnp.float32)
            for a in range(count):
                for b in range(DEV // 2):
                    fat = 256 * a + E * b
                    for h in range(2):
                        at = 256 * (i // 2 * count + a) + E * b + 8 * h
                        both = jnp.concatenate(
                            [logs[at : at + 8, 0:LANES], logs[at : at + 8, LANES : 2 * LANES]], axis=0
                        )
                        scaled = both * factor[fat : fat + E, LANES * h : LANES * h + LANES]
                        obuf[c, a, i + h, :, LANES * b : LANES * b + LANES] = scaled.astype(jnp.bfloat16)
        for a in range(count):
            pltpu.make_async_copy(obuf.at[c, a], finals[a].at[pl.ds(c * STEP, STEP)], osem).start()
        return carry

    lax.fori_loop(0, STEPS, step, 0)
    pltpu.make_async_copy(obuf, obuf, osem).wait()


def decode(wire, count, router=False, near=False):
    hbm = pl.BlockSpec(memory_space=pl.ANY)
    vmem = pl.BlockSpec(memory_space=pltpu.VMEM)
    final = jax.ShapeDtypeStruct((FD, E, DEV * M), jnp.bfloat16)
    scale = jax.ShapeDtypeStruct((E, FD), jnp.float32)
    row = jax.ShapeDtypeStruct((E, DEV * M), jnp.bfloat16)
    local = [
        pltpu.VMEM((STEPS, count, DEV, STEP * 8, LANES), jnp.bfloat16),
        pltpu.VMEM((DEV, wire.shape[1] - count * ROWS, LANES), jnp.bfloat16),
        pltpu.SemaphoreType.DMA((STEPS,)),
        pltpu.SemaphoreType.DMA,
    ]
    return pl.pallas_call(
        functools.partial(decode_kernel, count=count, router=router, near=near),
        in_specs=[vmem if near else hbm],
        out_specs=[hbm] * count + [vmem] * (count + router),
        out_shape=[final] * count + [scale] * count + [row] * router,
        scratch_shapes=[
            pltpu.VMEM((STEPS, count, STEP, E, DEV * M), jnp.bfloat16),
            pltpu.VMEM((256 * count, 256), jnp.bfloat16),
            pltpu.VMEM((256, 256), jnp.int32),
            pltpu.VMEM((256, 256), jnp.bfloat16),
            pltpu.SemaphoreType.DMA,
            *([] if near else local),
        ],
        compiler_params=pltpu.CompilerParams(vmem_limit_bytes=24 * 2**20),
        name="decode",
    )(wire)


def collect_kernel(*refs):
    *rows, out = refs
    me = lax.axis_index("expert")
    for k, row in enumerate(rows):
        at = pl.multiple_of(lax.rem(me + k, len(rows)) * E, E)
        out[pl.ds(at, E), :] = row[...]


def collect(row):
    size = lax.axis_size("expert")
    rows = [row]
    for k in range(1, size):
        rows.append(lax.ppermute(row, "expert", [((i + k) % size, i) for i in range(size)]))
    vmem = pl.BlockSpec(memory_space=pltpu.VMEM)
    return pl.pallas_call(
        collect_kernel,
        in_specs=[vmem] * size,
        out_specs=vmem,
        out_shape=jax.ShapeDtypeStruct((size * E, row.shape[1]), row.dtype),
        compiler_params=pltpu.CompilerParams(vmem_limit_bytes=4 * 2**20),
        name="collect",
    )(*rows)


def body(master_gate, master_up, master_down, router_weight, router_gain):
    first = encode((master_gate, master_up), (router_weight.T, router_gain[None, :]))
    second = encode((jnp.swapaxes(master_down, 1, 2),))
    first = lax.all_to_all(first, "shard", 0, 0, tiled=True)
    second = lax.all_to_all(second, "shard", 0, 0, tiled=True)
    gate, up, sgate, sup, row = decode(first, 2, True)
    router = collect(row)
    down, sdown = decode(second, 1, near=True)
    return (
        jnp.transpose(gate, (1, 2, 0)),
        jnp.transpose(up, (1, 2, 0)),
        jnp.transpose(down, (1, 0, 2)),
        sgate,
        sup,
        sdown,
        router.T,
    )


def solution(mesh):
    return jax.shard_map(
        body,
        mesh=mesh,
        in_specs=(
            P("expert", "shard", None),
            P("expert", "shard", None),
            P("expert", None, "shard"),
            P("shard", "expert"),
            P("shard"),
        ),
        out_specs=(
            P("expert", None, "shard"),
            P("expert", None, "shard"),
            P("expert", "shard", None),
            P("expert", "shard"),
            P("expert", "shard"),
            P("expert", "shard"),
            P(),
        ),
        check_vma=False,
    )
```

```python
import functools

import jax
import jax.numpy as jnp
from jax import lax
from jax.experimental import pallas as pl
from jax.experimental.pallas import tpu as pltpu
from jax.sharding import PartitionSpec as P


SPAN = 125.0
TINY = 1e-30
E = 16
F = 1408
M = 64
FD = 44
DEV = 32
LANES = 128
ROWS = FD * 8
PITCH = 9
VMEM = 56 * 2**20


def iota(shape, dim):
    return lax.broadcasted_iota(jnp.int32, shape, dim)


def partner(me, k, way):
    z, x, core = k // 8, k // 2 % 4, k % 2
    if way < 0:
        z, x = -z % 4, -x % 4
    return (me // 8 + z) % 4 * 8 + (me // 2 % 4 + x) % 4 * 2 + (me % 2 + core) % 2


def encode_kernel(*refs, count, router, apart):
    xs, refs = refs[:count], refs[count:]
    if router:
        weight, gain, refs = refs[0], refs[1], refs[2:]
    wires = DEV if apart else 1
    wire, refs = refs[:wires], refs[wires:]
    xbuf, scr0, scr1, packed, tops, meta, isem, osem, msem, *refs = refs
    spans = [(at, min(256, F - at)) for at in range(0, F, 256)]

    def brought(a, i):
        part = pl.ds(*spans[i])
        return pltpu.make_async_copy(xs[a].at[:, :, part], xbuf.at[a, :, :, part], isem.at[a, i])

    for a in range(count):
        for i in range(len(spans)):
            brought(a, i).start()
    if router:
        wbuf, gbuf, wsem, gsem = refs
        wcopy = pltpu.make_async_copy(weight, wbuf, wsem)
        gcopy = pltpu.make_async_copy(gain, gbuf, gsem)
        wcopy.start()
        gcopy.start()
    eye = (iota((256, 256), 0) == iota((256, 256), 1)).astype(jnp.bfloat16)

    def code(a, at, width, scr):
        for p in range(0, 8, 2):
            rows = []
            for e in (p, p + 8, p + 1, p + 9):
                v = xbuf[a, e, :, at : at + width]
                top = jnp.maximum(jnp.max(jnp.abs(v), axis=0, keepdims=True), TINY)
                tops[a, e : e + 1, at : at + width] = top
                rows.append(jnp.exp2(v * (SPAN / top)).astype(jnp.bfloat16))
            turned = lax.dot_general(
                eye[:width, :width],
                jnp.concatenate(rows, axis=0),
                (((1,), (1,)), ((), ())),
                preferred_element_type=jnp.float32,
            )
            for n in range(width // LANES):
                for q in range(2):
                    scr[pl.ds(n * LANES * PITCH + p + q, LANES, stride=PITCH), :] = turned[
                        LANES * n : LANES * n + LANES, LANES * q : LANES * q + LANES
                    ]

    def pack(a, at, width, scr):
        for f in range(0, width, 2):
            pair = [scr[PITCH * g : PITCH * g + 8, :] for g in (f, f + 1)]
            packed[a, 8 * (at + f) : 8 * (at + f) + 16, :] = jnp.concatenate(pair, axis=0).astype(jnp.bfloat16)
        for d in () if apart else range(at // FD, (at + width) // FD):
            pltpu.make_async_copy(
                packed.at[a, pl.ds(d * ROWS, ROWS), :], wire[0].at[d, pl.ds(a * ROWS, ROWS), :], osem
            ).start()

    def whole(a):
        last = None
        for i, (at, width) in enumerate(spans):
            brought(a, i).wait()
            scr = (scr0, scr1)[i % 2]
            code(a, at, width, scr)
            if last is not None:
                pack(*last)
            last = (a, at, width, scr)
        pack(*last)

    lane = iota((E, LANES), 1)

    for a in range(count):
        whole(a)
        for d in range(DEV):
            j, off = divmod(FD * d, LANES)
            near = tops[a, :, LANES * j : LANES * j + LANES]
            near = pltpu.roll(near, LANES - off, 1) if off else near
            if off + FD > LANES:
                far = pltpu.roll(tops[a, :, LANES * j + LANES : LANES * j + 2 * LANES], LANES - off, 1)
                near = jnp.where(lane < LANES - off, near, far)
            high = near.astype(jnp.bfloat16).astype(jnp.float32)
            rest = pltpu.roll(near - high, FD, 1)
            meta[d, E * a : E * a + E, :] = jnp.where(lane < FD, high, rest).astype(jnp.bfloat16)
    if router:
        wcopy.wait()
        gcopy.wait()
        r = wbuf[...] * gbuf[...]
        tile = jnp.concatenate([r[0:8], r[8:16]], axis=1).astype(jnp.bfloat16)
        for d in range(DEV):
            meta[d, E * count : E * count + 8, :] = tile
    rows = meta.shape[1]
    if apart:
        me = lax.axis_index("shard")
        for k in range(DEV):
            d = partner(me, k, 1)
            part = pl.ds(pl.multiple_of(d * ROWS, 16), ROWS)
            pltpu.make_async_copy(packed.at[0, part, :], wire[k].at[pl.ds(0, ROWS), :], osem).start()
            pltpu.make_async_copy(meta.at[d], wire[k].at[pl.ds(ROWS, rows), :], msem).start()
    else:
        pltpu.make_async_copy(meta, wire[0].at[:, pl.ds(count * ROWS, rows), :], msem).start()
    pltpu.make_async_copy(packed, packed, osem).wait()
    pltpu.make_async_copy(meta, meta, msem).wait()


def encode(xs, router=(), apart=False):
    count = len(xs)
    rows = E * count + (8 if router else 0)
    hbm = pl.BlockSpec(memory_space=pl.ANY)
    small = [pltpu.VMEM(r.shape, r.dtype) for r in router] + [pltpu.SemaphoreType.DMA] * len(router)
    return pl.pallas_call(
        functools.partial(encode_kernel, count=count, router=bool(router), apart=apart),
        in_specs=[hbm] * (count + len(router)),
        out_specs=[hbm] * (DEV if apart else 1),
        out_shape=[jax.ShapeDtypeStruct((ROWS + rows, LANES), jnp.bfloat16)] * DEV
        if apart
        else [jax.ShapeDtypeStruct((DEV, count * ROWS + rows, LANES), jnp.bfloat16)],
        scratch_shapes=[
            pltpu.VMEM((count, E, M, F), jnp.float32),
            pltpu.VMEM((256 * PITCH, LANES), jnp.float32),
            pltpu.VMEM((256 * PITCH, LANES), jnp.float32),
            pltpu.VMEM((count, F * 8, LANES), jnp.bfloat16),
            pltpu.VMEM((count, E, F), jnp.float32),
            pltpu.VMEM((DEV, rows, LANES), jnp.bfloat16),
            pltpu.SemaphoreType.DMA((count, pl.cdiv(F, 256))),
            pltpu.SemaphoreType.DMA,
            pltpu.SemaphoreType.DMA,
            *small,
        ],
        compiler_params=pltpu.CompilerParams(vmem_limit_bytes=VMEM),
        name="encode",
    )(*xs, *router)


STEP = 4
STEPS = FD // STEP


def decode_kernel(*refs, count, router, apart):
    wires = DEV if apart else 1
    wire, refs = refs[:wires], refs[wires:]
    finals, scales, refs = refs[:count], refs[count : 2 * count], refs[2 * count :]
    if router:
        routed, refs = refs[0], refs[1:]
    obuf, share, select, order, osem, *refs = refs
    tail = count * ROWS
    me = lax.axis_index("shard")
    if apart:
        base = tail
        odd = lax.rem(me, 2)
    else:
        odd = 0
        rbuf, mbuf, isem, msem = refs
        base = 0
        wire = wire[0]
        meta_copy = pltpu.make_async_copy(wire.at[:, pl.ds(tail, mbuf.shape[1]), :], mbuf, msem)
        meta_copy.start()
        for c in range(STEPS):
            for a in range(count):
                part = pl.ds(a * ROWS + c * STEP * 8, STEP * 8)
                pltpu.make_async_copy(wire.at[:, part, :], rbuf.at[c, a], isem.at[c]).start()
    k, n = iota((256, 256), 0), iota((256, 256), 1)
    source = (n & 63) + jnp.where((n & 64) == 0, 0, LANES) + jnp.where(n < LANES, 0, M)
    order[...] = jnp.where(k == lax.bitwise_xor(source, LANES * odd), 1.0, 0.0).astype(jnp.bfloat16)
    select[...] = (k & 127) - jnp.where((n & 64) == 0, 0, M) - jnp.where(n < LANES, 0, 1)
    if not apart:
        meta_copy.wait()

    def top_of(s, a):
        rows = pl.ds(base + E * a, E)
        v = (wire[s][rows, :] if apart else mbuf[s, rows, :]).astype(jnp.float32)
        return v + pltpu.roll(v, LANES - FD, 1)

    low = iota((E, LANES), 1) < M
    for a in range(count):
        top = top_of(0, a)
        for s in range(1, DEV):
            top = jnp.maximum(top, top_of(s, a))
        scales[a][...] = top[:, :FD]
        inv = 1.0 / (SPAN * jnp.maximum(top, TINY))
        for b in range(DEV // 2):
            one = top_of(2 * b, a) * inv
            two = top_of(2 * b + 1, a) * inv
            if apart:
                one, two = jnp.where(odd == 0, one, two), jnp.where(odd == 0, two, one)
            part = jnp.where(low, one, pltpu.roll(two, M, 1))
            high = part.astype(jnp.bfloat16)
            at = 256 * a + E * b
            share[at : at + E, 0:LANES] = high
            share[at : at + E, LANES : 2 * LANES] = (part - high.astype(jnp.float32)).astype(jnp.bfloat16)
    if router:
        at = base + E * count
        for b in range(DEV // 2):
            one = mbuf[2 * b, at : at + 8, :].astype(jnp.float32)
            two = mbuf[2 * b + 1, at : at + 8, :].astype(jnp.float32)
            first = jnp.where(low[0:8], one, pltpu.roll(two, M, 1))
            second = jnp.where(low[0:8], pltpu.roll(one, M, 1), two)
            routed[:, LANES * b : LANES * b + LANES] = jnp.concatenate([first, second], axis=0).astype(jnp.bfloat16)

    def codes_of(c, a, i, s):
        if apart:
            return wire[s][pl.ds(pl.multiple_of(a * ROWS + 8 * (c * STEP + i), 16), 16), :]
        return rbuf[c, a, s, 8 * i : 8 * i + 16, :]

    def place(b):
        if apart:
            return pl.ds(pl.multiple_of(LANES * lax.div(partner(me, 2 * b, -1), 2), LANES), LANES)
        return slice(LANES * b, LANES * b + LANES)

    def step(c, carry):
        if not apart:
            pltpu.make_async_copy(rbuf.at[c], rbuf.at[c], isem.at[c]).wait()
        rows = [
            jnp.concatenate([codes_of(c, a, i, 2 * b + q) for q in range(2)], axis=1)
            for i in range(0, STEP, 2)
            for a in range(count)
            for b in range(DEV // 2)
        ]
        logs = jnp.log2(jnp.dot(jnp.concatenate(rows, axis=0), order[...], preferred_element_type=jnp.float32))
        for i in range(0, STEP, 2):
            pick = jnp.where(select[...] == c * STEP + i, 1.0, 0.0).astype(jnp.bfloat16)
            factor = jnp.dot(share[...], pick, preferred_element_type=jnp.float32)
            for a in range(count):
                for b in range(DEV // 2):
                    fat = 256 * a + E * b
                    for h in range(2):
                        at = 256 * (i // 2 * count + a) + E * b + 8 * h
                        both = jnp.concatenate(
                            [logs[at : at + 8, 0:LANES], logs[at : at + 8, LANES : 2 * LANES]], axis=0
                        )
                        scaled = both * factor[fat : fat + E, LANES * h : LANES * h + LANES]
                        obuf[c, a, i + h, :, place(b)] = scaled.astype(jnp.bfloat16)
        for a in range(count):
            pltpu.make_async_copy(obuf.at[c, a], finals[a].at[pl.ds(c * STEP, STEP)], osem).start()
        return carry

    lax.fori_loop(0, STEPS, step, 0)
    pltpu.make_async_copy(obuf, obuf, osem).wait()


def decode(wire, count, router=False, apart=False):
    hbm = pl.BlockSpec(memory_space=pl.ANY)
    vmem = pl.BlockSpec(memory_space=pltpu.VMEM)
    final = jax.ShapeDtypeStruct((FD, E, DEV * M), jnp.bfloat16)
    scale = jax.ShapeDtypeStruct((E, FD), jnp.float32)
    row = jax.ShapeDtypeStruct((E, DEV * M), jnp.bfloat16)
    local = [] if apart else [
        pltpu.VMEM((STEPS, count, DEV, STEP * 8, LANES), jnp.bfloat16),
        pltpu.VMEM((DEV, wire[0].shape[1] - count * ROWS, LANES), jnp.bfloat16),
        pltpu.SemaphoreType.DMA((STEPS,)),
        pltpu.SemaphoreType.DMA,
    ]
    return pl.pallas_call(
        functools.partial(decode_kernel, count=count, router=router, apart=apart),
        in_specs=[vmem] * DEV if apart else [hbm],
        out_specs=[hbm] * count + [vmem] * (count + router),
        out_shape=[final] * count + [scale] * count + [row] * router,
        scratch_shapes=[
            pltpu.VMEM((STEPS, count, STEP, E, DEV * M), jnp.bfloat16),
            pltpu.VMEM((256 * count, 256), jnp.bfloat16),
            pltpu.VMEM((256, 256), jnp.int32),
            pltpu.VMEM((256, 256), jnp.bfloat16),
            pltpu.SemaphoreType.DMA,
            *local,
        ],
        compiler_params=pltpu.CompilerParams(vmem_limit_bytes=24 * 2**20),
        name="decode",
    )(*wire)


def collect_kernel(*refs):
    *rows, out = refs
    me = lax.axis_index("expert")
    for k, row in enumerate(rows):
        at = pl.multiple_of(lax.rem(me + k, len(rows)) * E, E)
        out[pl.ds(at, E), :] = row[...]


def collect(row):
    size = lax.axis_size("expert")
    rows = [row]
    for k in range(1, size):
        rows.append(lax.ppermute(row, "expert", [((i + k) % size, i) for i in range(size)]))
    vmem = pl.BlockSpec(memory_space=pltpu.VMEM)
    return pl.pallas_call(
        collect_kernel,
        in_specs=[vmem] * size,
        out_specs=vmem,
        out_shape=jax.ShapeDtypeStruct((size * E, row.shape[1]), row.dtype),
        compiler_params=pltpu.CompilerParams(vmem_limit_bytes=4 * 2**20),
        name="collect",
    )(*rows)


def hops():
    order = [(0, 0), (0, 1), (1, 0), (0, 3), (3, 0), (1, 1), (3, 3), (3, 1), (1, 3), (0, 2), (2, 0)]
    order += [(2, 1), (1, 2), (2, 3), (3, 2), (2, 2)]
    return [8 * z + 2 * x + core for core in (1, 0) for z, x in order if z + x + core]


def body(master_gate, master_up, master_down, router_weight, router_gain):
    (first,) = encode((master_gate, master_up), (router_weight.T, router_gain[None, :]))
    second = list(encode((jnp.swapaxes(master_down, 1, 2),), apart=True))
    first = lax.all_to_all(first, "shard", 0, 0, tiled=True)
    for k in hops():
        second[k] = lax.ppermute(second[k], "shard", [(i, partner(i, k, 1)) for i in range(DEV)])
    gate, up, sgate, sup, row = decode([first], 2, True)
    router = collect(row)
    down, sdown = decode(second, 1, apart=True)
    return (
        jnp.transpose(gate, (1, 2, 0)),
        jnp.transpose(up, (1, 2, 0)),
        jnp.transpose(down, (1, 0, 2)),
        sgate,
        sup,
        sdown,
        router.T,
    )


def solution(mesh):
    return jax.shard_map(
        body,
        mesh=mesh,
        in_specs=(
            P("expert", "shard", None),
            P("expert", "shard", None),
            P("expert", None, "shard"),
            P("shard", "expert"),
            P("shard"),
        ),
        out_specs=(
            P("expert", None, "shard"),
            P("expert", None, "shard"),
            P("expert", "shard", None),
            P("expert", "shard"),
            P("expert", "shard"),
            P("expert", "shard"),
            P(),
        ),
        check_vma=False,
    )
```
